512 devices in a mesh: fsdp: 64 (over y, x, z_lo), tp: 8 (over z_hi, core).
Axes of the slice: x: 4, y: 8, z: 8 (z_hi: 4, z_lo: 2; z = z_hi * 2 + z_lo), core: 2. Of those that a mesh axis runs over, the one named last changes fastest.
Arguments:
- saved_master: float32 [16384, 5120], P(('fsdp', 'tp')), may hold values from -6 to 6
- saved_first: float32 [16384, 5120], P(('fsdp', 'tp')), may hold values from -6 to 6
- saved_second: float32 [16384, 5120], P(('fsdp', 'tp')), may hold values from 0.05 to 20
- grad: bfloat16 [16384, 5120], P('fsdp', 'tp'), may hold values from -10000 to 10000
- row_target: int32 [16384], replicated, may hold values from 0 to 16383, as said below
- step: int32 [1], replicated, may hold values from 1 to 63
Outputs:
- new_master: float32 [16384, 5120], P('fsdp', 'tp')
- new_first: float32 [16384, 5120], P('fsdp', 'tp')
- new_second: float32 [16384, 5120], P('fsdp', 'tp')
- direction: float32 [16384, 5120], P('fsdp', 'tp')
The draws below stay inside these ranges and needn't reach their ends.
Inputs may be any that keep to these rules, and one draw needn't show every extreme that they name: `row_target`: a permutation of 0 to 16383; the saved rows j * 256 to (j + 1) * 256 - 1 of every block j send exactly 4 rows into every new block of 256 rows.
All inputs are finite; a program needn't handle non-finite values.
Results may differ from the reference program's by a relative error of at most 0.0003.
Values sent between devices are 32-bit elements; how exact they have to be, the bound alone decides.
A program may use at most 64 MiB of HBM per device.

```python
import math
import jax
import jax.numpy as jnp

H = 16384
D = 5120
N_FSDP = 64


def draw_row_target(key, part):
    block_rows = H // N_FSDP
    pair_rows = block_rows // N_FSDP
    source_keys = jax.random.split(jax.random.fold_in(key, 11), N_FSDP)
    target_keys = jax.random.split(jax.random.fold_in(key, 12), N_FSDP)
    sigma = jax.vmap(lambda one: jax.random.permutation(one, block_rows))(source_keys).astype(jnp.int32)
    tau_table = jax.vmap(lambda one: jax.random.permutation(one, block_rows))(target_keys).astype(jnp.int32)
    target_block = sigma // pair_rows
    slot_index = sigma % pair_rows
    incoming = jnp.arange(N_FSDP, dtype=jnp.int32)[:, None] * pair_rows + slot_index
    local_row = tau_table.reshape(-1)[target_block * block_rows + incoming]
    return (target_block * block_rows + local_row).reshape(-1).astype(jnp.int32)


def draw_grad(key, part):
    row_key = jax.random.fold_in(key, 21)
    col_key = jax.random.fold_in(key, 22)
    base_key = jax.random.fold_in(key, 23)
    rising = 1.0 + 2.0 * jnp.arange(H, dtype=jnp.float32) / (H - 1)
    row_scale = jnp.exp(jax.random.uniform(row_key, (H, 1)) * math.log(10.0)) * rising[:, None]
    col_scale = jnp.exp(jax.random.uniform(col_key, (1, D)) * math.log(10.0))
    values = jax.random.normal(base_key, (H, D))
    return (values * row_scale * col_scale).astype(jnp.bfloat16)


def level_of(key, extent, cuts, low, largest):
    factor_of, own = 1.0, jax.random.fold_in(key, 6)
    for position, shards_of in cuts:
        heights = jnp.exp(jax.random.uniform(jax.random.fold_in(own, position), (shards_of,), jnp.float32, low / len(cuts), largest / len(cuts)))
        factor_of = factor_of * jnp.repeat(heights, extent[position] // shards_of).reshape([-1 if axis == position else 1 for axis in range(len(extent))])
    return factor_of


def scatter_about(stream_key, dims, deviation, reach, cuts=(), kind=jnp.bfloat16):
    array = jax.random.normal(stream_key, dims, jnp.float32) * deviation
    if len(cuts) > 0:
        array = level_of(stream_key, dims, cuts, -0.22, 0.18) * array
    return jnp.clip(array, min=-reach, max=reach).astype(kind)


def setup_inputs(seed: int = 0) -> dict:
    key_list = jax.random.split(jax.random.key(seed), 7)
    saved_master = scatter_about(key_list[0], (H, D), 1.0, 6.0, ((0, 512),), jnp.float32)
    saved_first = scatter_about(key_list[1], (H, D), 1.0, 6.0, ((0, 512),), jnp.float32)
    saved_second = jnp.clip(jnp.exp(math.log(20.0) - 5.9914645 * jax.random.uniform(key_list[2], (H, D), jnp.float32) ** level_of(key_list[2], (H, D), ((0, 512),), -0.2, 0.2)), 0.05, 20.0)
    grad = draw_grad(jax.random.fold_in(key_list[6], 71), 0)
    row_target = draw_row_target(jax.random.fold_in(key_list[6], 71), 0)
    step = jax.random.randint(key_list[5], (1,), 1, 64).astype(jnp.int32)
    return dict(saved_master=saved_master, saved_first=saved_first, saved_second=saved_second, grad=grad, row_target=row_target, step=step)


beta_one = 0.9
beta_two = 0.95
epsilon = 1e-08
learn_rate = 0.001
weight_decay = 0.1

def adam_update(master, first, second, grad, scale, step):
    clipped = scale * grad.astype(jnp.float32)
    first_new = beta_one * first + (1.0 - beta_one) * clipped
    second_new = beta_two * second + (1.0 - beta_two) * clipped * clipped
    count = step[0].astype(jnp.float32)
    first_hat = first_new / (1.0 - jnp.power(jnp.float32(beta_one), count))
    second_hat = second_new / (1.0 - jnp.power(jnp.float32(beta_two), count))
    direction = first_hat / (jnp.sqrt(second_hat) + epsilon) + weight_decay * master
    return (master - learn_rate * direction, first_new, second_new, direction)

def reference(saved_master, saved_first, saved_second, grad, row_target, step):
    master = jnp.zeros_like(saved_master).at[row_target].set(saved_master)
    first = jnp.zeros_like(saved_first).at[row_target].set(saved_first)
    second = jnp.zeros_like(saved_second).at[row_target].set(saved_second)
    grad_wide = grad.astype(jnp.float32)
    total = jnp.sum(grad_wide * grad_wide)
    scale = jnp.minimum(1.0, math.sqrt(H * D) / jnp.sqrt(total))
    return adam_update(master, first, second, grad, scale, step)
```

```python
import functools
import math

import jax
import jax.numpy as jnp
from jax import lax
from jax.experimental import pallas as pl
from jax.experimental.pallas import tpu as pltpu
from jax.sharding import PartitionSpec as P

H = 16384
D = 5120
F = 64
T = 8
N_Y, N_X, N_Z = 8, 4, 2
ROWS = H // F
PIECE = ROWS // T
COLS = D // T
LANES = 128
PER = COLS // LANES
BLOCKS = 3 * PER
UNITS = (BLOCKS + 1) // 2
SLOTS = 8 * F

beta_one = 0.9
beta_two = 0.95
epsilon = 1e-08
learn_rate = 0.001
weight_decay = 0.1

MESH = pl.DeviceIdType.MESH
F32, BF16, I32 = jnp.float32, jnp.bfloat16, jnp.int32


def two_parts(x):
    high = x.astype(BF16)
    low = (x - high.astype(F32)).astype(BF16)
    return jnp.concatenate([high, low], axis=1)


def moved(order, x):
    both = jnp.dot(order, two_parts(x), preferred_element_type=F32)
    return both[:, :LANES] + both[:, LANES:]


def fsdp_peer(me, i):
    y, x, z = me // (N_X * N_Z), me // N_Z % N_X, me % N_Z
    y = (y + i // (N_X * N_Z)) % N_Y
    x = (x + i // N_Z % N_X) % N_X
    z = (z + i % N_Z) % N_Z
    return (y * N_X + x) * N_Z + z


def tp_peer(me, i):
    return (me // 2 + i // 2) % 4 * 2 + (me + i) % 2


def kernel(
    master, first, second, grad, targets, out, total,
    whole, leaving, arrived, sums_out, sums, wide, to_slot, to_row,
    own_sem, sum_sem, tp_sem, fsdp_sem, sum_sent, tp_sent, fsdp_sent,
):
    f, t = lax.axis_index("fsdp"), lax.axis_index("tp")
    barrier = pltpu.get_barrier_semaphore()

    def greet_tp(i, carry):
        pl.semaphore_signal(barrier, inc=1, device_id=(f, tp_peer(t, i)), device_id_type=MESH)
        return carry

    def greet_fsdp(i, carry):
        pl.semaphore_signal(barrier, inc=1, device_id=(fsdp_peer(f, i), t), device_id_type=MESH)
        return carry

    lax.fori_loop(1, T, greet_tp, 0)
    lax.fori_loop(1, F, greet_fsdp, 0)

    saved = (master, first, second)
    here = pl.ds(pl.multiple_of(t * PIECE, PIECE), PIECE)
    own = []
    for b in range(BLOCKS):
        a, c = divmod(b, PER)
        at = pl.multiple_of(t * COLS + c * LANES, LANES)
        copy = pltpu.make_async_copy(saved[a].at[:, pl.ds(at, LANES)], whole.at[b, here, :], own_sem.at[b])
        copy.start()
        own.append(copy)

    square = jnp.zeros((8, LANES), F32)
    for c in range(PER):
        wide_grad = grad[:, c * LANES : (c + 1) * LANES].astype(F32)
        square += jnp.sum((wide_grad * wide_grad).reshape(ROWS // 8, 8, LANES), axis=0)
    sums_out[...] = square
    mine_sum = pl.ds(pl.multiple_of(t * 8, 8), 8)
    sums[mine_sum, :] = square

    pl.semaphore_wait(barrier, F + T - 2)

    def send_sum(i, carry):
        pltpu.make_async_remote_copy(
            src_ref=sums_out, dst_ref=sums.at[mine_sum, :], send_sem=sum_sent, recv_sem=sum_sem,
            device_id=(f, tp_peer(t, i)), device_id_type=MESH,
        ).start()
        return carry

    for b in range(BLOCKS):
        a, c = divmod(b, PER)

        def send_piece(i, carry, a=a, b=b, c=c):
            other = tp_peer(t, i)
            at = pl.multiple_of(other * COLS + c * LANES, LANES)
            pltpu.make_async_remote_copy(
                src_ref=saved[a].at[:, pl.ds(at, LANES)], dst_ref=whole.at[b, here, :],
                send_sem=tp_sent, recv_sem=tp_sem.at[b],
                device_id=(f, other), device_id_type=MESH,
            ).start()
            return carry

        lax.fori_loop(1, T, send_piece, 0)
        if b == 1:
            lax.fori_loop(1, T, send_sum, 0)

    mine = jnp.concatenate([targets[pl.ds(2 * f, 1), :], targets[pl.ds(2 * f + 1, 1), :]], axis=1).astype(F32)
    across = jnp.broadcast_to(mine, (ROWS, ROWS))
    slot = jnp.sum(jnp.where(across.T < across, 1.0, 0.0), axis=0, keepdims=True)
    line = lax.broadcasted_iota(I32, (SLOTS, 2 * ROWS), 0)
    lane = lax.broadcasted_iota(I32, (SLOTS, 2 * ROWS), 1)
    line_key = line // 8 * 4 + line % 4 + line // 4 % 2 * 1024
    slot_key = jnp.concatenate([slot, slot + 1024.0], axis=1)
    to_slot[...] = jnp.where(line_key.astype(F32) == slot_key, 1.0, 0.0).astype(BF16)

    def widen(s, carry):
        at = pl.ds(pl.multiple_of(8 * s, 8), 8)
        wide[at, :LANES] = jnp.broadcast_to(targets[pl.ds(2 * s, 1), :], (8, LANES))
        wide[at, LANES:] = jnp.broadcast_to(targets[pl.ds(2 * s + 1, 1), :], (8, LANES))
        return carry

    lax.fori_loop(0, F, widen, 0)
    left = jnp.where(wide[...] // ROWS == f, wide[...] % ROWS, 4096).astype(F32)
    nth = lax.broadcasted_iota(I32, (SLOTS, 1), 0)
    row = jnp.zeros((SLOTS, 1), F32)
    for n in range(4):
        least = jnp.min(left, axis=1, keepdims=True)
        row = jnp.where(nth % 4 == n, least, row)
        if n < 3:
            left = jnp.where(left == least, 4096.0, left)
    row_key = row + (nth // 4 % 2 * 1024).astype(F32)
    lane_key = (lane % ROWS + lane // ROWS * 1024).astype(F32)
    to_row[...] = jnp.where(row_key == lane_key, 1.0, 0.0).T.astype(BF16)

    for copy in own:
        copy.wait()
    pltpu.make_async_copy(sums.at[pl.ds(0, 8 * (T - 1)), :], sums.at[pl.ds(0, 8 * (T - 1)), :], sum_sem).wait()
    whole[BLOCKS, :, :] = jnp.broadcast_to(jnp.sum(sums[...], axis=0, keepdims=True), (ROWS, LANES))

    others = ROWS - PIECE
    to_me = pl.ds(pl.multiple_of(8 * f, 8), 8)

    def send_unit(u, carry):
        def arrive(b):
            part = whole.at[b, pl.ds(0, others), :]
            pltpu.make_async_copy(part, part, tp_sem.at[b]).wait()

        arrive(2 * u)

        @pl.when(2 * u + 1 < BLOCKS)
        def _():
            arrive(2 * u + 1)

        both = jnp.concatenate([whole[2 * u], whole[2 * u + 1]], axis=0)
        leaving[u] = moved(to_slot[...], both)
        arrived[u, to_me, :] = leaving[u, to_me, :]

        def send(i, carry):
            other = fsdp_peer(f, i)
            pltpu.make_async_remote_copy(
                src_ref=leaving.at[u, pl.ds(pl.multiple_of(8 * other, 8), 8), :],
                dst_ref=arrived.at[u, to_me, :],
                send_sem=fsdp_sent, recv_sem=fsdp_sem.at[u],
                device_id=(other, t), device_id_type=MESH,
            ).start()
            return carry

        lax.fori_loop(1, F, send, 0)
        return carry

    lax.fori_loop(0, UNITS, send_unit, 0)

    def place_unit(u, carry):
        part = arrived.at[u, pl.ds(0, SLOTS - 8), :]
        pltpu.make_async_copy(part, part, fsdp_sem.at[u]).wait()
        both = moved(to_row[...], arrived[u])

        def put(b, value):
            out[b // PER, :, pl.ds(pl.multiple_of(b % PER * LANES, LANES), LANES)] = value

        put(2 * u, both[:ROWS])

        @pl.when(2 * u + 1 < BLOCKS)
        def _():
            put(2 * u + 1, both[ROWS:])

        @pl.when(2 * u + 1 == BLOCKS)
        def _():
            total[...] = jnp.broadcast_to(0.25 * jnp.sum(both[ROWS:]), (8, LANES))

        return carry

    lax.fori_loop(0, UNITS, place_unit, 0)

    pltpu.make_async_copy(sums.at[pl.ds(0, 8 * (T - 1)), :], sums.at[pl.ds(0, 8 * (T - 1)), :], sum_sent).wait()
    sent = whole.at[pl.ds(0, BLOCKS), pl.ds(0, others), :]
    pltpu.make_async_copy(sent, sent, tp_sent).wait()
    sent = leaving.at[:, pl.ds(0, SLOTS - 8), :]
    pltpu.make_async_copy(sent, sent, fsdp_sent).wait()


def restore(saved_master, saved_first, saved_second, grad, targets):
    vmem = pl.BlockSpec(memory_space=pltpu.VMEM)
    anywhere = pl.BlockSpec(memory_space=pl.ANY)
    dma = pltpu.SemaphoreType.DMA
    return pl.pallas_call(
        kernel,
        out_shape=(
            jax.ShapeDtypeStruct((3, ROWS, COLS), F32),
            jax.ShapeDtypeStruct((8, LANES), F32),
        ),
        in_specs=[anywhere, anywhere, anywhere, vmem, vmem],
        out_specs=(vmem, vmem),
        scratch_shapes=[
            pltpu.VMEM((BLOCKS + 1, ROWS, LANES), F32),
            pltpu.VMEM((UNITS, SLOTS, LANES), F32),
            pltpu.VMEM((UNITS, SLOTS, LANES), F32),
            pltpu.VMEM((8, LANES), F32),
            pltpu.VMEM((8 * T, LANES), F32),
            pltpu.VMEM((SLOTS, 2 * LANES), I32),
            pltpu.VMEM((SLOTS, SLOTS), BF16),
            pltpu.VMEM((SLOTS, SLOTS), BF16),
            dma((BLOCKS,)),
            dma,
            dma((BLOCKS,)),
            dma((UNITS,)),
            dma,
            dma,
            dma,
        ],
        name="restore",
        compiler_params=pltpu.CompilerParams(
            collective_id=0, has_side_effects=True, vmem_limit_bytes=48 * 1024 * 1024
        ),
    )(saved_master, saved_first, saved_second, grad, targets)


def adam_update(master, first, second, grad, scale, step):
    clipped = scale * grad.astype(jnp.float32)
    first_new = beta_one * first + (1.0 - beta_one) * clipped
    second_new = beta_two * second + (1.0 - beta_two) * clipped * clipped
    count = step[0].astype(jnp.float32)
    first_hat = first_new / (1.0 - jnp.power(jnp.float32(beta_one), count))
    second_hat = second_new / (1.0 - jnp.power(jnp.float32(beta_two), count))
    direction = first_hat / (jnp.sqrt(second_hat) + epsilon) + weight_decay * master
    return (master - learn_rate * direction, first_new, second_new, direction)


def per_device(saved_master, saved_first, saved_second, grad, row_target, step):
    targets = row_target.reshape(H // LANES, LANES)
    state, total = restore(saved_master, saved_first, saved_second, grad, targets)
    scale = jnp.minimum(1.0, math.sqrt(H * D) / jnp.sqrt(total[0, 0]))
    return adam_update(state[0], state[1], state[2], grad, scale, step)


def solution(mesh):
    in_specs = (
        P(("fsdp", "tp"), None),
        P(("fsdp", "tp"), None),
        P(("fsdp", "tp"), None),
        P("fsdp", "tp"),
        P(),
        P(),
    )
    out_specs = (P("fsdp", "tp"), P("fsdp", "tp"), P("fsdp", "tp"), P("fsdp", "tp"))
    return jax.shard_map(
        per_device, mesh=mesh, in_specs=in_specs, out_specs=out_specs, check_vma=False
    )
```

```python
import functools
import math

import jax
import jax.numpy as jnp
from jax import lax
from jax.experimental import pallas as pl
from jax.experimental.pallas import tpu as pltpu
from jax.sharding import PartitionSpec as P

H = 16384
D = 5120
F = 64
T = 8
N_Y, N_X, N_Z = 8, 4, 2
ROWS = H // F
PIECE = ROWS // T
COLS = D // T
LANES = 128
PER = COLS // LANES
BLOCKS = 3 * PER + 1
SLOTS = 8 * F
LIMIT = math.sqrt(H * D)

beta_one = 0.9
beta_two = 0.95
epsilon = 1e-08
learn_rate = 0.001
weight_decay = 0.1

MESH = pl.DeviceIdType.MESH
F32, BF16, I32 = jnp.float32, jnp.bfloat16, jnp.int32
scope = jax.named_scope


def two_parts(x):
    high = x.astype(BF16)
    low = (x - high.astype(F32)).astype(BF16)
    return jnp.concatenate([high, low], axis=1)


def moved(order, x):
    both = jnp.dot(order, two_parts(x), preferred_element_type=F32)
    return both[:, :LANES] + both[:, LANES:]


def fsdp_peer(me, dy, dx, dz):
    y, x, z = me // (N_X * N_Z), me // N_Z % N_X, me % N_Z
    return ((y + dy) % N_Y * N_X + (x + dx) % N_X) * N_Z + (z + dz) % N_Z


def tp_peer(me, i):
    return (me // 2 + i // 2) % 4 * 2 + (me + i) % 2


def kernel(
    master, first, second, grad_in, targets_in, out, clipped,
    stage, grad, targets, whole, leaving, arrived, sums_out, sums, row_sum, row_sums, wide, to_slot, to_row,
    local_sem, own_sem, sum_sem, tp_sem, row_sem, fsdp_sem, sum_sent, tp_sent, row_sent, fsdp_sent, x_sem, z_sem,
):
    f, t = lax.axis_index("fsdp"), lax.axis_index("tp")
    barrier = pltpu.get_barrier_semaphore()

    def signal(semaphore, at):
        pl.semaphore_signal(semaphore, inc=1, device_id=at, device_id_type=MESH)

    arrived[0] = jnp.zeros((SLOTS, LANES), F32)
    row_sums[...] = jnp.zeros((SLOTS, LANES), F32)
    with scope("greet"):
        for dz in range(1, N_Z):
            signal(barrier, (fsdp_peer(f, 0, 0, dz), t))
        for dx in range(1, N_X):
            signal(barrier, (fsdp_peer(f, 0, dx, 0), t))
        for i in range(1, T):
            signal(barrier, (f, tp_peer(t, i)))
        for dy in range(1, N_Y):
            signal(barrier, (fsdp_peer(f, dy, 0, 0), t))

    with scope("local"):
        saved = (master, first, second)
        here = pl.ds(pl.multiple_of(t * PIECE, PIECE), PIECE)
        loads = []
        for a in range(3):
            copy = pltpu.make_async_copy(saved[a], stage.at[a], local_sem.at[a])
            copy.start()
            loads.append(copy)
        grad_load = pltpu.make_async_copy(grad_in, grad, local_sem.at[3])
        grad_load.start()
        target_load = pltpu.make_async_copy(targets_in, targets, local_sem.at[4])
        target_load.start()
        own = []
        for b in range(1, BLOCKS):
            a, c = divmod(b - 1, PER)
            at = pl.multiple_of(t * COLS + c * LANES, LANES)
            copy = pltpu.make_async_copy(saved[a].at[:, pl.ds(at, LANES)], whole.at[b, here, :], own_sem.at[b])
            copy.start()
            own.append(copy)
        loads[0].wait()

    with scope("barrier"):
        pl.semaphore_wait(barrier, (N_Y - 1) + (N_X - 1) + (N_Z - 1) + (T - 1))

    def send_block(b):
        a, c = (b - 1) // PER, (b - 1) % PER
        for i in range(1, T):
            other = tp_peer(t, i)
            at = pl.multiple_of(other * COLS + c * LANES, LANES)
            pltpu.make_async_remote_copy(
                src_ref=stage.at[a, :, pl.ds(at, LANES)], dst_ref=whole.at[b, here, :],
                send_sem=tp_sent, recv_sem=tp_sem.at[b],
                device_id=(f, other), device_id_type=MESH,
            ).start()

    with scope("issueA0"):
        send_block(1)
        for dx in range(1, N_X):
            signal(x_sem, (fsdp_peer(f, 0, dx, 0), t))
        grad_load.wait()
        square = jnp.zeros((8, LANES), F32)
        for c in range(PER):
            wide_grad = grad[:, c * LANES : (c + 1) * LANES].astype(F32)
            square += jnp.sum((wide_grad * wide_grad).reshape(ROWS // 8, 8, LANES), axis=0)
        sums_out[...] = square
        mine_sum = pl.ds(pl.multiple_of(t * 8, 8), 8)
        sums[mine_sum, :] = square
        for i in range(1, T):
            pltpu.make_async_remote_copy(
                src_ref=sums_out, dst_ref=sums.at[mine_sum, :], send_sem=sum_sent, recv_sem=sum_sem,
                device_id=(f, tp_peer(t, i)), device_id_type=MESH,
            ).start()

        def send_blocks(b, carry):
            send_block(b)
            return carry

        for a in range(3):
            if a > 0:
                loads[a].wait()
            lax.fori_loop(max(2, 1 + a * PER), 1 + (a + 1) * PER, send_blocks, 0)

    with scope("slots"):
        target_load.wait()
        mine = jnp.concatenate([targets[pl.ds(2 * f, 1), :], targets[pl.ds(2 * f + 1, 1), :]], axis=1).astype(F32)
        across = jnp.broadcast_to(mine, (ROWS, ROWS))
        slot = jnp.sum(jnp.where(across.T < across, 1.0, 0.0), axis=0, keepdims=True)
        line = lax.broadcasted_iota(I32, (SLOTS, 1), 0)
        slot_line = line // 8 * 4 + line % 4
        for h in range(2):
            key = jnp.where(line // 4 % 2 == h, slot_line, -1).astype(F32)
            to_slot[h] = jnp.where(key == slot, 1.0, 0.0).astype(BF16)

    with scope("barrier2"):
        pl.semaphore_wait(x_sem, N_X - 1)
        for dz in range(1, N_Z):
            signal(z_sem, (fsdp_peer(f, 0, 0, dz), t))
    with scope("own"):
        for copy in own:
            copy.wait()
    with scope("waitsum"):
        some = sums.at[pl.ds(0, 8 * (T - 1)), :]
        pltpu.make_async_copy(some, some, sum_sem).wait()
        row_sum[...] = jnp.broadcast_to(jnp.sum(sums[...], axis=0, keepdims=True), (8, LANES))
        row_sums[pl.ds(pl.multiple_of(8 * f, 8), 8), :] = row_sum[...]
    with scope("barrier3"):
        pl.semaphore_wait(z_sem, N_Z - 1)

    others = ROWS - PIECE

    def send(b, dy, dx, dz):
        other = fsdp_peer(f, dy, dx, dz)
        half = b % 2 * 4
        pltpu.make_async_remote_copy(
            src_ref=leaving.at[b, pl.ds(pl.multiple_of(8 * other + half, 4), 4), :],
            dst_ref=arrived.at[b // 2, pl.ds(pl.multiple_of(8 * f + half, 4), 4), :],
            send_sem=fsdp_sent, recv_sem=fsdp_sem.at[b],
            device_id=(other, t), device_id_type=MESH,
        ).start()

    def keep(b):
        half = b % 2 * 4
        arrived[b // 2, pl.ds(pl.multiple_of(8 * f + half, 4), 4), :] = (
            leaving[b, pl.ds(pl.multiple_of(8 * f + half, 4), 4), :])

    def send_all(b):
        def send_line(dy, carry):
            for dx in range(N_X):
                for dz in range(N_Z):
                    send(b, dy, dx, dz)
            return carry

        lax.fori_loop(1, N_Y, send_line, 0)
        for dx in range(N_X):
            for dz in range(N_Z):
                if dx or dz:
                    send(b, 0, dx, dz)

    def send_row_sum(i, carry):
        other = fsdp_peer(f, i // (N_X * N_Z), i // N_Z % N_X, i % N_Z)
        pltpu.make_async_remote_copy(
            src_ref=row_sum.at[pl.ds(0, 1), :],
            dst_ref=row_sums.at[pl.ds(pl.multiple_of(8 * f, 8), 1), :],
            send_sem=row_sent, recv_sem=row_sem,
            device_id=(other, t), device_id_type=MESH,
        ).start()
        return carry

    with scope("issueS"):
        lax.fori_loop(1, F, send_row_sum, 0)

    def send_step(b, carry):
        with scope("waitA"):
            part = whole.at[b, pl.ds(0, others), :]
            pltpu.make_async_copy(part, part, tp_sem.at[b]).wait()
        leaving[b] = moved(to_slot[b % 2], whole[b])
        keep(b)

        with scope("issueB"):
            send_all(b)

        @pl.when(b == 2)
        def _():
            with scope("rows"):
                def widen(s, carry):
                    at = pl.ds(pl.multiple_of(8 * s, 8), 8)
                    wide[at, :LANES] = jnp.broadcast_to(targets[pl.ds(2 * s, 1), :], (8, LANES))
                    wide[at, LANES:] = jnp.broadcast_to(targets[pl.ds(2 * s + 1, 1), :], (8, LANES))
                    return carry

                lax.fori_loop(0, F, widen, 0)
                left = jnp.where(wide[...] // ROWS == f, wide[...] % ROWS, 4096).astype(F32)
                nth = lax.broadcasted_iota(I32, (SLOTS, 1), 0)
                row = jnp.zeros((SLOTS, 1), F32)
                for n in range(4):
                    least = jnp.min(left, axis=1, keepdims=True)
                    row = jnp.where(nth % 4 == n, least, row)
                    if n < 3:
                        left = jnp.where(left == least, 4096.0, left)
                row_key = row + (nth // 4 % 2 * 1024).astype(F32)
                lanes = lax.broadcasted_iota(I32, (SLOTS, SLOTS), 1)
                lane_key = (lanes % ROWS + lanes // ROWS * 1024).astype(F32)
                to_row[...] = jnp.where(row_key == lane_key, 1.0, 0.0).T.astype(BF16)

        return carry

    lax.fori_loop(1, BLOCKS, send_step, 0)

    def put(b, value):
        at = pl.ds(pl.multiple_of((b - 1) % PER * LANES, LANES), LANES)
        out[(b - 1) // PER, :, at] = value

    def place_unit(u, carry):
        with scope("waitB"):
            part = arrived.at[0, pl.ds(0, (SLOTS - 8) // 2), :]

            @pl.when(u > 0)
            def _():
                pltpu.make_async_copy(part, part, fsdp_sem.at[2 * u]).wait()

            pltpu.make_async_copy(part, part, fsdp_sem.at[2 * u + 1]).wait()
        both = moved(to_row[...], arrived[u])

        @pl.when(u > 0)
        def _():
            put(2 * u, both[:ROWS])

        put(2 * u + 1, both[ROWS:])
        return carry

    with scope("clip"):
        some = row_sums.at[pl.ds(0, F - 1), :]
        pltpu.make_async_copy(some, some, row_sem).wait()
        first_line = lax.broadcasted_iota(I32, (SLOTS, LANES), 0) % 8 == 0
        total = jnp.sum(jnp.where(first_line, row_sums[...], 0.0), axis=0, keepdims=True)
        total = jnp.sum(total, axis=1, keepdims=True)
        scale = jnp.minimum(1.0, LIMIT / jnp.sqrt(total))
        clipped[...] = scale * grad[...].astype(F32)

    lax.fori_loop(0, BLOCKS // 2, place_unit, 0)

    with scope("sent"):
        some = sums.at[pl.ds(0, 8 * (T - 1)), :]
        pltpu.make_async_copy(some, some, sum_sent).wait()
        sent = whole.at[pl.ds(1, BLOCKS - 1), pl.ds(0, others), :]
        pltpu.make_async_copy(sent, sent, tp_sent).wait()
        sent = leaving.at[pl.ds(1, BLOCKS - 1), pl.ds(0, (SLOTS - 8) // 2), :]
        pltpu.make_async_copy(sent, sent, fsdp_sent).wait()
        some = row_sums.at[pl.ds(0, F - 1), :]
        pltpu.make_async_copy(some, some, row_sent).wait()


def restore(saved_master, saved_first, saved_second, grad, targets):
    hbm = pl.BlockSpec(memory_space=pltpu.HBM)
    vmem = pl.BlockSpec(memory_space=pltpu.VMEM)
    given = (saved_master, saved_first, saved_second, grad, targets)
    dma = pltpu.SemaphoreType.DMA
    regular = pltpu.SemaphoreType.REGULAR
    return pl.pallas_call(
        kernel,
        out_shape=(
            jax.ShapeDtypeStruct((3, ROWS, COLS), F32),
            jax.ShapeDtypeStruct((ROWS, COLS), F32),
        ),
        in_specs=[hbm] * 5,
        out_specs=(vmem, vmem),
        scratch_shapes=[
            pltpu.VMEM((3, PIECE, D), F32),
            pltpu.VMEM((ROWS, COLS), BF16),
            pltpu.VMEM((H // LANES, LANES), I32),
            pltpu.VMEM((BLOCKS, ROWS, LANES), F32),
            pltpu.VMEM((BLOCKS, SLOTS, LANES), F32),
            pltpu.VMEM((BLOCKS // 2, SLOTS, LANES), F32),
            pltpu.VMEM((8, LANES), F32),
            pltpu.VMEM((8 * T, LANES), F32),
            pltpu.VMEM((8, LANES), F32),
            pltpu.VMEM((SLOTS, LANES), F32),
            pltpu.VMEM((SLOTS, 2 * LANES), I32),
            pltpu.VMEM((2, SLOTS, ROWS), BF16),
            pltpu.VMEM((SLOTS, SLOTS), BF16),
            dma((5,)),
            dma((BLOCKS,)),
            dma,
            dma((BLOCKS,)),
            dma,
            dma((BLOCKS,)),
            dma,
            dma,
            dma,
            dma,
            regular,
            regular,
        ],
        name="restore",
        compiler_params=pltpu.CompilerParams(
            collective_id=0, has_side_effects=True, vmem_limit_bytes=32 * 1024 * 1024
        ),
    )(*(pltpu.with_memory_space_constraint(x, pltpu.HBM) for x in given))


def adam_update(master, first, second, clipped, step):
    first_new = beta_one * first + (1.0 - beta_one) * clipped
    second_new = beta_two * second + (1.0 - beta_two) * clipped * clipped
    count = step[0].astype(jnp.float32)
    first_hat = first_new / (1.0 - jnp.power(jnp.float32(beta_one), count))
    second_hat = second_new / (1.0 - jnp.power(jnp.float32(beta_two), count))
    direction = first_hat / (jnp.sqrt(second_hat) + epsilon) + weight_decay * master
    return (master - learn_rate * direction, first_new, second_new, direction)


def per_device(saved_master, saved_first, saved_second, grad, row_target, step):
    targets = row_target.reshape(H // LANES, LANES)
    state, clipped = restore(saved_master, saved_first, saved_second, grad, targets)
    return adam_update(state[0], state[1], state[2], clipped, step)


def solution(mesh):
    in_specs = (
        P(("fsdp", "tp"), None),
        P(("fsdp", "tp"), None),
        P(("fsdp", "tp"), None),
        P("fsdp", "tp"),
        P(),
        P(),
    )
    out_specs = (P("fsdp", "tp"), P("fsdp", "tp"), P("fsdp", "tp"), P("fsdp", "tp"))
    return jax.shard_map(
        per_device, mesh=mesh, in_specs=in_specs, out_specs=out_specs, check_vma=False
    )
```

```python
import functools
import math

import jax
import jax.numpy as jnp
from jax import lax
from jax.experimental import pallas as pl
from jax.experimental.pallas import tpu as pltpu
from jax.sharding import PartitionSpec as P

H = 16384
D = 5120
F = 64
T = 8
N_Y, N_X, N_Z = 8, 4, 2
ROWS = H // F
PIECE = ROWS // T
COLS = D // T
LANES = 128
PER = COLS // LANES
BLOCKS = 3 * PER + 1
SLOTS = 8 * F
LIMIT = math.sqrt(H * D)

beta_one = 0.9
beta_two = 0.95
epsilon = 1e-08
learn_rate = 0.001
weight_decay = 0.1

MESH = pl.DeviceIdType.MESH
F32, BF16, I32 = jnp.float32, jnp.bfloat16, jnp.int32
scope = jax.named_scope


def two_parts(x):
    high = x.astype(BF16)
    low = (x - high.astype(F32)).astype(BF16)
    return jnp.concatenate([high, low], axis=1)


def moved(order, x):
    both = jnp.dot(order, two_parts(x), preferred_element_type=F32)
    return both[:, :LANES] + both[:, LANES:]


def fsdp_peer(me, dy, dx, dz):
    y, x, z = me // (N_X * N_Z), me // N_Z % N_X, me % N_Z
    return ((y + dy) % N_Y * N_X + (x + dx) % N_X) * N_Z + (z + dz) % N_Z


def tp_peer(me, i):
    return (me // 2 + i // 2) % 4 * 2 + (me + i) % 2


def kernel(
    master, first, second, grad_in, targets_in, out, clipped,
    stage, grad, targets, whole, leaving, arrived, sums_out, sums, row_sum, row_sums, wide, to_slot, to_row,
    local_sem, own_sem, sum_sem, tp_sem, row_sem, fsdp_sem, sum_sent, tp_sent, row_sent, fsdp_sent, x_sem, z_sem,
):
    f, t = lax.axis_index("fsdp"), lax.axis_index("tp")
    barrier = pltpu.get_barrier_semaphore()

    def signal(semaphore, at):
        pl.semaphore_signal(semaphore, inc=1, device_id=at, device_id_type=MESH)

    arrived[0] = jnp.zeros((SLOTS, LANES), F32)
    row_sums[...] = jnp.zeros((SLOTS, LANES), F32)
    with scope("greet"):
        for dz in range(1, N_Z):
            signal(barrier, (fsdp_peer(f, 0, 0, dz), t))
        for dx in range(1, N_X):
            signal(barrier, (fsdp_peer(f, 0, dx, 0), t))
        for i in range(1, T):
            signal(barrier, (f, tp_peer(t, i)))
        for dy in range(1, N_Y):
            signal(barrier, (fsdp_peer(f, dy, 0, 0), t))

    with scope("local"):
        saved = (master, first, second)
        here = pl.ds(pl.multiple_of(t * PIECE, PIECE), PIECE)
        loads = []
        for a in range(3):
            copy = pltpu.make_async_copy(saved[a], stage.at[a], local_sem.at[a])
            copy.start()
            loads.append(copy)
        grad_load = pltpu.make_async_copy(grad_in, grad, local_sem.at[3])
        grad_load.start()
        target_load = pltpu.make_async_copy(targets_in, targets, local_sem.at[4])
        target_load.start()
        own = []
        for b in range(1, BLOCKS):
            a, c = divmod(b - 1, PER)
            at = pl.multiple_of(t * COLS + c * LANES, LANES)
            copy = pltpu.make_async_copy(saved[a].at[:, pl.ds(at, LANES)], whole.at[b, here, :], own_sem.at[b])
            copy.start()
            own.append(copy)
        loads[0].wait()

    with scope("barrier"):
        pl.semaphore_wait(barrier, (N_Y - 1) + (N_X - 1) + (N_Z - 1) + (T - 1))

    def send_block(b):
        a, c = (b - 1) // PER, (b - 1) % PER
        for i in range(1, T):
            other = tp_peer(t, i)
            at = pl.multiple_of(other * COLS + c * LANES, LANES)
            pltpu.make_async_remote_copy(
                src_ref=stage.at[a, :, pl.ds(at, LANES)], dst_ref=whole.at[b, here, :],
                send_sem=tp_sent, recv_sem=tp_sem.at[b],
                device_id=(f, other), device_id_type=MESH,
            ).start()

    with scope("issueA0"):
        send_block(1)
        for dx in range(1, N_X):
            signal(x_sem, (fsdp_peer(f, 0, dx, 0), t))
        grad_load.wait()
        square = jnp.zeros((8, LANES), F32)
        for c in range(PER):
            wide_grad = grad[:, c * LANES : (c + 1) * LANES].astype(F32)
            square += jnp.sum((wide_grad * wide_grad).reshape(ROWS // 8, 8, LANES), axis=0)
        sums_out[...] = square
        mine_sum = pl.ds(pl.multiple_of(t * 8, 8), 8)
        sums[mine_sum, :] = square
        for i in range(1, T):
            pltpu.make_async_remote_copy(
                src_ref=sums_out, dst_ref=sums.at[mine_sum, :], send_sem=sum_sent, recv_sem=sum_sem,
                device_id=(f, tp_peer(t, i)), device_id_type=MESH,
            ).start()

        def send_blocks(b, carry):
            send_block(b)
            return carry

        for a in range(3):
            if a > 0:
                loads[a].wait()
            lax.fori_loop(max(2, 1 + a * PER), 1 + (a + 1) * PER, send_blocks, 0)

    with scope("slots"):
        target_load.wait()
        mine = jnp.concatenate([targets[pl.ds(2 * f, 1), :], targets[pl.ds(2 * f + 1, 1), :]], axis=1).astype(F32)
        across = jnp.broadcast_to(mine, (ROWS, ROWS))
        slot = jnp.sum(jnp.where(across.T < across, 1.0, 0.0), axis=0, keepdims=True)
        line = lax.broadcasted_iota(I32, (SLOTS, 1), 0)
        slot_line = line // 8 * 4 + line % 4
        for h in range(2):
            key = jnp.where(line // 4 % 2 == h, slot_line, -1).astype(F32)
            to_slot[h] = jnp.where(key == slot, 1.0, 0.0).astype(BF16)

    with scope("barrier2"):
        pl.semaphore_wait(x_sem, N_X - 1)
        for dz in range(1, N_Z):
            signal(z_sem, (fsdp_peer(f, 0, 0, dz), t))
    with scope("own"):
        for copy in own:
            copy.wait()
    with scope("waitsum"):
        some = sums.at[pl.ds(0, 8 * (T - 1)), :]
        pltpu.make_async_copy(some, some, sum_sem).wait()
        row_sum[...] = jnp.broadcast_to(jnp.sum(sums[...], axis=0, keepdims=True), (8, LANES))
        row_sums[pl.ds(pl.multiple_of(8 * f, 8), 8), :] = row_sum[...]
    with scope("barrier3"):
        pl.semaphore_wait(z_sem, N_Z - 1)

    others = ROWS - PIECE

    def send(b, dy, dx, dz):
        other = fsdp_peer(f, dy, dx, dz)
        half = b % 2 * 4
        pltpu.make_async_remote_copy(
            src_ref=leaving.at[b, pl.ds(pl.multiple_of(8 * other + half, 4), 4), :],
            dst_ref=arrived.at[b // 2, pl.ds(pl.multiple_of(8 * f + half, 4), 4), :],
            send_sem=fsdp_sent, recv_sem=fsdp_sem.at[b],
            device_id=(other, t), device_id_type=MESH,
        ).start()

    def keep(b):
        half = b % 2 * 4
        arrived[b // 2, pl.ds(pl.multiple_of(8 * f + half, 4), 4), :] = (
            leaving[b, pl.ds(pl.multiple_of(8 * f + half, 4), 4), :])

    def to_all(send_one):
        def send_line(i, carry):
            dy = N_Y // 2 + (i + 1) // 2 * (1 - 2 * (i % 2))
            for dx in (2, 1, 3, 0):
                for dz in (1, 0):
                    send_one(dy, dx, dz)
            return carry

        lax.fori_loop(0, N_Y - 1, send_line, 0)
        for dx in (2, 1, 3, 0):
            for dz in (1, 0):
                if dx or dz:
                    send_one(0, dx, dz)

    def send_all(b):
        to_all(lambda dy, dx, dz: send(b, dy, dx, dz))

    def send_row_sum(dy, dx, dz):
        pltpu.make_async_remote_copy(
            src_ref=row_sum.at[pl.ds(0, 1), :],
            dst_ref=row_sums.at[pl.ds(pl.multiple_of(8 * f, 8), 1), :],
            send_sem=row_sent, recv_sem=row_sem,
            device_id=(fsdp_peer(f, dy, dx, dz), t), device_id_type=MESH,
        ).start()

    with scope("issueS"):
        to_all(send_row_sum)

    def send_step(b, carry):
        with scope("waitA"):
            part = whole.at[b, pl.ds(0, others), :]
            pltpu.make_async_copy(part, part, tp_sem.at[b]).wait()
        leaving[b] = moved(to_slot[b % 2], whole[b])
        keep(b)

        with scope("issueB"):
            send_all(b)

        @pl.when(b == 2)
        def _():
            with scope("rows"):
                def widen(s, carry):
                    at = pl.ds(pl.multiple_of(8 * s, 8), 8)
                    wide[at, :LANES] = jnp.broadcast_to(targets[pl.ds(2 * s, 1), :], (8, LANES))
                    wide[at, LANES:] = jnp.broadcast_to(targets[pl.ds(2 * s + 1, 1), :], (8, LANES))
                    return carry

                lax.fori_loop(0, F, widen, 0)
                left = jnp.where(wide[...] // ROWS == f, wide[...] % ROWS, 4096).astype(F32)
                nth = lax.broadcasted_iota(I32, (SLOTS, 1), 0)
                row = jnp.zeros((SLOTS, 1), F32)
                for n in range(4):
                    least = jnp.min(left, axis=1, keepdims=True)
                    row = jnp.where(nth % 4 == n, least, row)
                    if n < 3:
                        left = jnp.where(left == least, 4096.0, left)
                row_key = row + (nth // 4 % 2 * 1024).astype(F32)
                lanes = lax.broadcasted_iota(I32, (SLOTS, SLOTS), 1)
                lane_key = (lanes % ROWS + lanes // ROWS * 1024).astype(F32)
                to_row[...] = jnp.where(row_key == lane_key, 1.0, 0.0).T.astype(BF16)

        return carry

    lax.fori_loop(1, BLOCKS, send_step, 0)

    def put(b, value):
        at = pl.ds(pl.multiple_of((b - 1) % PER * LANES, LANES), LANES)
        out[(b - 1) // PER, :, at] = value

    def place_unit(u, carry):
        with scope("waitB"):
            part = arrived.at[0, pl.ds(0, (SLOTS - 8) // 2), :]

            @pl.when(u > 0)
            def _():
                pltpu.make_async_copy(part, part, fsdp_sem.at[2 * u]).wait()

            pltpu.make_async_copy(part, part, fsdp_sem.at[2 * u + 1]).wait()
        both = moved(to_row[...], arrived[u])

        @pl.when(u > 0)
        def _():
            put(2 * u, both[:ROWS])

        put(2 * u + 1, both[ROWS:])
        return carry

    with scope("clip"):
        some = row_sums.at[pl.ds(0, F - 1), :]
        pltpu.make_async_copy(some, some, row_sem).wait()
        first_line = lax.broadcasted_iota(I32, (SLOTS, LANES), 0) % 8 == 0
        total = jnp.sum(jnp.where(first_line, row_sums[...], 0.0), axis=0, keepdims=True)
        total = jnp.sum(total, axis=1, keepdims=True)
        scale = jnp.minimum(1.0, LIMIT / jnp.sqrt(total))
        clipped[...] = scale * grad[...].astype(F32)

    lax.fori_loop(0, BLOCKS // 2, place_unit, 0)

    with scope("sent"):
        some = sums.at[pl.ds(0, 8 * (T - 1)), :]
        pltpu.make_async_copy(some, some, sum_sent).wait()
        sent = whole.at[pl.ds(1, BLOCKS - 1), pl.ds(0, others), :]
        pltpu.make_async_copy(sent, sent, tp_sent).wait()
        sent = leaving.at[pl.ds(1, BLOCKS - 1), pl.ds(0, (SLOTS - 8) // 2), :]
        pltpu.make_async_copy(sent, sent, fsdp_sent).wait()
        some = row_sums.at[pl.ds(0, F - 1), :]
        pltpu.make_async_copy(some, some, row_sent).wait()


def restore(saved_master, saved_first, saved_second, grad, targets):
    hbm = pl.BlockSpec(memory_space=pltpu.HBM)
    vmem = pl.BlockSpec(memory_space=pltpu.VMEM)
    given = (saved_master, saved_first, saved_second, grad, targets)
    dma = pltpu.SemaphoreType.DMA
    regular = pltpu.SemaphoreType.REGULAR
    return pl.pallas_call(
        kernel,
        out_shape=(
            jax.ShapeDtypeStruct((3, ROWS, COLS), F32),
            jax.ShapeDtypeStruct((ROWS, COLS), F32),
        ),
        in_specs=[hbm] * 5,
        out_specs=(vmem, vmem),
        scratch_shapes=[
            pltpu.VMEM((3, PIECE, D), F32),
            pltpu.VMEM((ROWS, COLS), BF16),
            pltpu.VMEM((H // LANES, LANES), I32),
            pltpu.VMEM((BLOCKS, ROWS, LANES), F32),
            pltpu.VMEM((BLOCKS, SLOTS, LANES), F32),
            pltpu.VMEM((BLOCKS // 2, SLOTS, LANES), F32),
            pltpu.VMEM((8, LANES), F32),
            pltpu.VMEM((8 * T, LANES), F32),
            pltpu.VMEM((8, LANES), F32),
            pltpu.VMEM((SLOTS, LANES), F32),
            pltpu.VMEM((SLOTS, 2 * LANES), I32),
            pltpu.VMEM((2, SLOTS, ROWS), BF16),
            pltpu.VMEM((SLOTS, SLOTS), BF16),
            dma((5,)),
            dma((BLOCKS,)),
            dma,
            dma((BLOCKS,)),
            dma,
            dma((BLOCKS,)),
            dma,
            dma,
            dma,
            dma,
            regular,
            regular,
        ],
        name="restore",
        compiler_params=pltpu.CompilerParams(
            collective_id=0, has_side_effects=True, vmem_limit_bytes=32 * 1024 * 1024
        ),
    )(*(pltpu.with_memory_space_constraint(x, pltpu.HBM) for x in given))


def adam_update(master, first, second, clipped, step):
    first_new = beta_one * first + (1.0 - beta_one) * clipped
    second_new = beta_two * second + (1.0 - beta_two) * clipped * clipped
    count = step[0].astype(jnp.float32)
    first_hat = first_new / (1.0 - jnp.power(jnp.float32(beta_one), count))
    second_hat = second_new / (1.0 - jnp.power(jnp.float32(beta_two), count))
    direction = first_hat / (jnp.sqrt(second_hat) + epsilon) + weight_decay * master
    return (master - learn_rate * direction, first_new, second_new, direction)


def per_device(saved_master, saved_first, saved_second, grad, row_target, step):
    targets = row_target.reshape(H // LANES, LANES)
    state, clipped = restore(saved_master, saved_first, saved_second, grad, targets)
    return adam_update(state[0], state[1], state[2], clipped, step)


def solution(mesh):
    in_specs = (
        P(("fsdp", "tp"), None),
        P(("fsdp", "tp"), None),
        P(("fsdp", "tp"), None),
        P("fsdp", "tp"),
        P(),
        P(),
    )
    out_specs = (P("fsdp", "tp"), P("fsdp", "tp"), P("fsdp", "tp"), P("fsdp", "tp"))
    return jax.shard_map(
        per_device, mesh=mesh, in_specs=in_specs, out_specs=out_specs, check_vma=False
    )
```
